32 devices in a mesh: groups: 2 (over y), ga: 16 (over z, x, core).
Axes of the slice: x: 2, y: 2, z: 4, core: 2. Of those that a mesh axis runs over, the one named last changes fastest.
Arguments:
- occupied: float32 [2, 1024, 12288], P(None, None, 'ga'), may hold values from -0.0546875 to 0.0546875
- residual: float32 [4, 2, 128, 12288], P('groups', None, None, 'ga'), parts along dimension 0, may hold values from -6 to 6
- old_direction: float32 [4, 2, 128, 12288], P('groups', None, None, 'ga'), parts along dimension 0, may hold values from -6 to 6
- kin_ratio: float32 [12288], P('ga'), may hold values from 0.06 to 5, as said below
- old_dot: float32 [4, 128], P('groups'), parts along dimension 0, may hold values from 6144 to 24576
Outputs:
- direction: float32 [4, 2, 128, 12288], P('groups', None, None, 'ga'), parts along dimension 0
- dot_new: float32 [4, 128], P('groups'), parts along dimension 0
The draws below stay inside these ranges and needn't reach their ends.
There are 2 independent parts, one for each index of `groups`. The reference program is written for one: setup_inputs(seed, part) draws one part's arguments, and reference() takes and returns one part's arrays. A program takes and returns all parts, laid end to end along the dimension named above; an argument that names none is the same for every part. Nothing has to cross between parts.
Inputs may be any that keep to these rules, and one draw needn't show every extreme that they name: `kin_ratio`: positive; grows with the plane-wave index on average and varies from one plane wave to the next.
All inputs are finite; a program needn't handle non-finite values.
Results may differ from the reference program's by a relative error of at most 0.000056.
Values sent between devices are 32-bit elements; how exact they have to be, the bound alone decides.
No kernel may reach another device: no remote copies, remote signals or barrier semaphores. Data moves between devices by JAX's collectives and lax.ppermute only.
A program may use at most 64 MiB of HBM per device.

```python
import math
import jax
import jax.numpy as jnp
from jax import lax

NOCC = 1024
NB = 128
P_SIZE = 2
NG = 12288


def draw_kin_ratio(key, part):
    position = jnp.arange(NG, dtype=jnp.float32) / NG
    baseline = 0.1 + 3.0 * position ** (2.0 / 3.0)
    roughness = jnp.exp(jax.random.uniform(key, (NG,), jnp.float32, -0.4, 0.4))
    return baseline * roughness


def levels(stream_key, dims, shards, smallest, largest):
    factor_of = 1.0
    for dim, shards_of in shards:
        heights = jax.random.uniform(jax.random.fold_in(jax.random.fold_in(stream_key, 6), dim), (shards_of,), jnp.float32, smallest / len(shards), largest / len(shards))
        factor_of = factor_of * jnp.repeat(jnp.exp(heights), dims[dim] // shards_of).reshape((-1,) + (1,) * (len(dims) - 1 - dim))
    return factor_of


def bell_draw(own_key, shape, scale, most, split=(), kind=jnp.bfloat16):
    drawn = jax.random.normal(own_key, shape, jnp.float32) * scale
    if len(split) > 0:
        drawn = levels(own_key, shape, split, -0.22, 0.18) * drawn
    return jnp.clip(drawn, min=-most, max=most).astype(kind)


def setup_inputs(seed: int = 0, part: int = 0) -> dict:
    splits = jax.random.split(jax.random.key(seed), 6)
    own_keys = jax.random.split(jax.random.fold_in(splits[5], part), 6)
    return {
        "occupied": bell_draw(splits[0], (2, NOCC, NG), NG ** -0.5, 0.0546875, ((2, 16),), jnp.float32),
        "residual": bell_draw(own_keys[1], (P_SIZE, 2, NB, NG), 1.0, 6.0, ((3, 16),), jnp.float32),
        "old_direction": bell_draw(own_keys[2], (P_SIZE, 2, NB, NG), 1.0, 6.0, ((3, 16),), jnp.float32),
        "kin_ratio": draw_kin_ratio(jax.random.fold_in(splits[5], 71), part),
        "old_dot": jnp.clip(jnp.exp(jax.random.uniform(own_keys[4], (P_SIZE, NB), jnp.float32, math.log(6144.0), math.log(24576.0))), 6144.0, 24576.0),
    }


highest = lax.Precision.HIGHEST


def teter_factor(ratio):
    numerator = 27.0 + 18.0 * ratio + 12.0 * ratio ** 2 + 8.0 * ratio ** 3
    return numerator / (numerator + 16.0 * ratio ** 4)


def margins(occupied, vectors):
    products = jnp.einsum("hng,pcbg->phcnb", occupied, vectors, precision=highest)
    real_part = products[:, 0, 0] + products[:, 1, 1]
    imag_part = products[:, 0, 1] - products[:, 1, 0]
    return jnp.stack([real_part, imag_part], axis=1)


def correction(summed, occ_rows):
    real_part = summed[:, 0]
    imag_part = summed[:, 1]
    coefficient = jnp.stack([jnp.stack([real_part, -imag_part], axis=1), jnp.stack([imag_part, real_part], axis=1)], axis=1)
    return jnp.einsum("pchnb,hng->pcbg", coefficient, occ_rows, precision=highest)


def reference(occupied, residual, old_direction, kin_ratio, old_dot):
    factor = teter_factor(kin_ratio)
    first = margins(occupied, residual)
    gradient = residual - correction(first, occupied)
    precond = factor * gradient
    dot_new = jnp.sum(factor * (gradient[:, 0] ** 2 + gradient[:, 1] ** 2), axis=-1)
    second = margins(occupied, precond)
    projected = precond - correction(second, occupied)
    direction = projected + (dot_new / old_dot)[:, None, :, None] * old_direction
    return direction, dot_new
```

```python
import jax
import jax.numpy as jnp
from jax import lax
from jax.sharding import PartitionSpec as P


high = lax.Precision.HIGH
AXIS = "ga"


def teter_factor(ratio):
    numerator = 27.0 + 18.0 * ratio + 12.0 * ratio**2 + 8.0 * ratio**3
    return numerator / (numerator + 16.0 * ratio**4)


def radices(size):
    digits, rest = [], size
    if rest % 2 == 0:
        digits.append(2)
        rest //= 2
    while rest > 1:
        step = 4 if (rest % 4 == 0 and rest.bit_length() % 2 == 1) else 2
        digits.append(step)
        rest //= step
    return digits


def swap(value, size, offset):
    return lax.ppermute(value, AXIS, [(i, i ^ offset) for i in range(size)])


def reduce_scatter(value, size):
    place = lax.axis_index(AXIS)
    stride = 1
    for radix in radices(size):
        digit = (place // stride) % radix
        rows = value.shape[0] // radix
        parts = value.reshape((radix, rows) + value.shape[1:])
        received = [
            swap(lax.dynamic_index_in_dim(parts, digit ^ k, 0, keepdims=False), size, k * stride)
            for k in range(1, radix)
        ]
        value = lax.dynamic_index_in_dim(parts, digit, 0, keepdims=False)
        for other in received:
            value = value + other
        stride *= radix
    return value


def all_gather(value, size):
    place = lax.axis_index(AXIS)
    stride = size
    for radix in reversed(radices(size)):
        stride //= radix
        digit = (place // stride) % radix
        pieces = [value] + [swap(value, size, k * stride) for k in range(1, radix)]
        ordered = []
        for slot in range(radix):
            piece = pieces[0]
            for k in range(1, radix):
                piece = jnp.where((digit ^ k) == slot, pieces[k], piece)
            ordered.append(piece)
        value = jnp.concatenate(ordered, axis=0)
    return value


def total(value, size):
    stride = 1
    for radix in radices(size):
        received = [swap(value, size, k * stride) for k in range(1, radix)]
        for other in received:
            value = value + other
        stride *= radix
    return value


def margins(occupied, vectors):
    dims = (((1,), (1,)), ((), ()))
    first = jnp.concatenate([vectors[0], vectors[1]], axis=0)
    second = jnp.concatenate([vectors[1], -vectors[0]], axis=0)
    return lax.dot_general(occupied[0], first, dims, precision=high) + lax.dot_general(
        occupied[1], second, dims, precision=high
    )


def correction(summed, occupied):
    dims = (((0,), (0,)), ((), ()))
    bands = summed.shape[1] // 2
    turned = jnp.concatenate([-summed[:, bands:], summed[:, :bands]], axis=1)
    out = lax.dot_general(summed, occupied[0], dims, precision=high) + lax.dot_general(
        turned, occupied[1], dims, precision=high
    )
    return out.reshape(2, bands, -1)


def on_device(size, occupied, residual, old_direction, kin_ratio, old_dot):
    factor = teter_factor(kin_ratio)
    count = residual.shape[0]
    sums = [reduce_scatter(margins(occupied, residual[p]), size) for p in range(count)]
    sums = [all_gather(s, size) for s in sums]
    gradient = [residual[p] - correction(sums[p], occupied) for p in range(count)]
    precond = [factor * g for g in gradient]
    local_dot = jnp.stack([jnp.sum(factor * (g[0] ** 2 + g[1] ** 2), axis=-1) for g in gradient])
    second = [reduce_scatter(margins(occupied, v), size) for v in precond]
    dot_new = total(local_dot, size)
    second = [all_gather(s, size) for s in second]
    scale = dot_new / old_dot
    direction = [
        precond[p] - correction(second[p], occupied) + scale[p][None, :, None] * old_direction[p]
        for p in range(count)
    ]
    return (jnp.stack(direction), dot_new)


def solution(mesh):
    size = mesh.shape[AXIS]
    placed = (
        P(None, None, "ga"),
        P("groups", None, None, "ga"),
        P("groups", None, None, "ga"),
        P("ga"),
        P("groups", None),
    )
    return jax.shard_map(
        lambda *args: on_device(size, *args),
        mesh=mesh,
        in_specs=placed,
        out_specs=(P("groups", None, None, "ga"), P("groups", None)),
        check_vma=False,
    )
```

```python
import jax
import jax.numpy as jnp
from jax import lax
from jax.sharding import PartitionSpec as P


high = lax.Precision.HIGH
AXIS = "ga"


def teter_factor(ratio):
    numerator = 27.0 + 18.0 * ratio + 12.0 * ratio**2 + 8.0 * ratio**3
    return numerator / (numerator + 16.0 * ratio**4)


def radices(size):
    digits, rest = [], size
    if rest % 2 == 0:
        digits.append(2)
        rest //= 2
    while rest > 1:
        step = 4 if (rest % 4 == 0 and rest.bit_length() % 2 == 1) else 2
        digits.append(step)
        rest //= step
    return digits


def swap(value, size, offset):
    return lax.ppermute(value, AXIS, [(i, i ^ offset) for i in range(size)])


def scatter_step(value, size, stride, radix):
    digit = (lax.axis_index(AXIS) // stride) % radix
    rows = value.shape[0] // radix
    parts = value.reshape((radix, rows) + value.shape[1:])
    received = [
        swap(lax.dynamic_index_in_dim(parts, digit ^ k, 0, keepdims=False), size, k * stride)
        for k in range(1, radix)
    ]
    value = lax.dynamic_index_in_dim(parts, digit, 0, keepdims=False)
    for other in received:
        value = value + other
    return value


def scatter_rest(value, size):
    stride = 1
    for place, radix in enumerate(radices(size)):
        if place > 0:
            value = scatter_step(value, size, stride, radix)
        stride *= radix
    return value


def scatter_first(value, size):
    digits = radices(size)
    return scatter_step(value, size, 1, digits[0]) if digits else value


def all_gather(value, size):
    place = lax.axis_index(AXIS)
    stride = size
    for radix in reversed(radices(size)):
        stride //= radix
        digit = (place // stride) % radix
        pieces = [value] + [swap(value, size, k * stride) for k in range(1, radix)]
        ordered = []
        for slot in range(radix):
            piece = pieces[0]
            for k in range(1, radix):
                piece = jnp.where((digit ^ k) == slot, pieces[k], piece)
            ordered.append(piece)
        value = jnp.concatenate(ordered, axis=0)
    return value


def total(value, size):
    stride = 1
    for radix in radices(size):
        received = [swap(value, size, k * stride) for k in range(1, radix)]
        for other in received:
            value = value + other
        stride *= radix
    return value


def margins(occupied, vectors):
    dims = (((1,), (1,)), ((), ()))
    first = jnp.concatenate([vectors[0], vectors[1]], axis=0)
    second = jnp.concatenate([vectors[1], -vectors[0]], axis=0)
    return lax.dot_general(occupied[0], first, dims, precision=high) + lax.dot_general(
        occupied[1], second, dims, precision=high
    )


def correction(summed, occupied):
    dims = (((0,), (0,)), ((), ()))
    bands = summed.shape[1] // 2
    turned = jnp.concatenate([-summed[:, bands:], summed[:, :bands]], axis=1)
    out = lax.dot_general(summed, occupied[0], dims, precision=high) + lax.dot_general(
        turned, occupied[1], dims, precision=high
    )
    return out.reshape(2, bands, -1)


def on_device(size, occupied, residual, old_direction, kin_ratio, old_dot):
    factor = teter_factor(kin_ratio)
    count = residual.shape[0]
    def after(value, *others):
        return lax.optimization_barrier((value,) + others)

    sums, vectors = [], [residual[p] for p in range(count)]
    for p in range(count):
        part = scatter_first(margins(occupied, vectors[p]), size)
        if p + 1 < count:
            vectors[p + 1], part = after(vectors[p + 1], part)
        sums.append(all_gather(scatter_rest(part, size), size))
    precond, local_dot, second = [], [], []
    for p in range(count):
        gradient = residual[p] - correction(sums[p], occupied)
        precond.append(factor * gradient)
        local_dot.append(jnp.sum(factor * (gradient[0] ** 2 + gradient[1] ** 2), axis=-1))
        vector = precond[p]
        if p > 0:
            vector, second[p - 1] = after(vector, second[p - 1])
        first = margins(occupied, vector)
        if p + 1 < count:
            sums[p + 1], first = after(sums[p + 1], first)
        second.append(scatter_first(first, size))
    dot_new = total(jnp.stack(local_dot), size)
    second = [all_gather(scatter_rest(s, size), size) for s in second]
    scale = dot_new / old_dot
    direction = [
        precond[p] - correction(second[p], occupied) + scale[p][None, :, None] * old_direction[p]
        for p in range(count)
    ]
    return (jnp.stack(direction), dot_new)


def solution(mesh):
    size = mesh.shape[AXIS]
    placed = (
        P(None, None, "ga"),
        P("groups", None, None, "ga"),
        P("groups", None, None, "ga"),
        P("ga"),
        P("groups", None),
    )
    return jax.shard_map(
        lambda *args: on_device(size, *args),
        mesh=mesh,
        in_specs=placed,
        out_specs=(P("groups", None, None, "ga"), P("groups", None)),
        check_vma=False,
    )
```
